8 devices in a mesh: dp: 1 (over z), fsdp: 2 (over y), ep: 4 (over x, core).
Axes of the slice: x: 2, y: 2, z: 1, core: 2. Of those that a mesh axis runs over, the one named last changes fastest.
Arguments:
- hidden: bfloat16 [32768, 1024], P(('dp', 'fsdp', 'ep'))
- norm_gain: bfloat16 [1024], replicated
- w_router: bfloat16 [1024, 32], replicated
- w_gate: bfloat16 [32, 1024, 2816], P('ep', 'fsdp')
- w_up: bfloat16 [32, 1024, 2816], P('ep', 'fsdp')
- w_down: bfloat16 [32, 2816, 1024], P('ep', None, 'fsdp')
- top2_ids: int32 [32768, 2], P(('dp', 'fsdp', 'ep'))
Outputs:
- output: bfloat16 [32768, 1024], P(('dp', 'fsdp', 'ep'))
All inputs are finite; a program needn't handle non-finite values.
Results may differ from the reference program's by a relative error of at most 0.001.
Values are sent between devices in bfloat16 or wider.
A program may use at most 1 GiB of HBM per device.

```python
import jax
import jax.numpy as jnp
import numpy as np
from jax import lax

D = 1024
FF = 2816
EXPERTS = 32
TOKENS_DEV = 4096
GROUPS = 8
TOKENS = GROUPS * TOKENS_DEV
CAPACITY = (5 * TOKENS_DEV + 2 * EXPERTS - 1) // (2 * EXPERTS)
EPS = 1e-5


def draw_routes(route_key):
    perm_key, first_key, second_key = jax.random.split(route_key, 3)
    hot_count = max(EXPERTS // 4, 1)
    route_table = jnp.asarray(np.repeat(np.arange(EXPERTS), np.where(np.arange(EXPERTS) < hot_count, 4, 1)), dtype=jnp.int32)
    expert_perm = jax.random.permutation(perm_key, EXPERTS)
    table_pick = jax.random.randint(first_key, (TOKENS,), 0, route_table.shape[0])
    local_index = jnp.arange(TOKENS, dtype=jnp.int32) % TOKENS_DEV
    first_choice = jnp.where(local_index < EXPERTS, local_index, expert_perm[route_table[table_pick]])
    second_shift = jax.random.randint(second_key, (TOKENS,), 1, EXPERTS)
    second_choice = (first_choice + second_shift) % EXPERTS
    return jnp.stack([first_choice, second_choice], axis=1).astype(jnp.int32)


def setup_inputs(seed: int = 0, part: int = 0) -> dict:
    part_key = jax.random.fold_in(jax.random.key(seed), part)
    hidden_key, route_key = jax.random.split(part_key, 2)
    gain_key, router_key, gate_key, up_key, down_key = jax.random.split(jax.random.key(seed + 1), 5)
    hidden = jax.random.normal(hidden_key, (TOKENS, D), jnp.float32)
    norm_gain = jax.random.uniform(gain_key, (D,), jnp.float32, 0.5, 1.5)
    w_router = jax.random.normal(router_key, (D, EXPERTS), jnp.float32) * (0.5 * D ** -0.5)
    w_gate = jax.random.normal(gate_key, (EXPERTS, D, FF), jnp.float32) * D ** -0.5
    w_up = jax.random.normal(up_key, (EXPERTS, D, FF), jnp.float32) * D ** -0.5
    w_down = jax.random.normal(down_key, (EXPERTS, FF, D), jnp.float32) * FF ** -0.5
    return {
        'hidden': hidden.astype(jnp.bfloat16),
        'norm_gain': norm_gain.astype(jnp.bfloat16),
        'w_router': w_router.astype(jnp.bfloat16),
        'w_gate': w_gate.astype(jnp.bfloat16),
        'w_up': w_up.astype(jnp.bfloat16),
        'w_down': w_down.astype(jnp.bfloat16),
        'top2_ids': draw_routes(route_key),
    }


def expert_ffn(expert_pack):
    rows_in, gate_mat, up_mat, down_mat = expert_pack
    act_a = jnp.dot(rows_in, gate_mat, preferred_element_type=jnp.float32)
    act_b = jnp.dot(rows_in, up_mat, preferred_element_type=jnp.float32)
    hidden_act = (jax.nn.silu(act_a) * act_b).astype(jnp.bfloat16)
    return jnp.dot(hidden_act, down_mat, preferred_element_type=jnp.float32).astype(jnp.bfloat16)


def reference(hidden, norm_gain, w_router, w_gate, w_up, w_down, top2_ids):
    hidden_f32 = hidden.astype(jnp.float32)
    mean_sq = jnp.mean(hidden_f32 * hidden_f32, axis=-1, keepdims=True)
    normed = (hidden_f32 * lax.rsqrt(mean_sq + EPS) * norm_gain.astype(jnp.float32)).astype(jnp.bfloat16)
    logits = jnp.dot(normed, w_router, preferred_element_type=jnp.float32)
    gate_probs = jax.nn.softmax(jnp.take_along_axis(logits, top2_ids, axis=1), axis=-1)
    flat_ids = top2_ids.reshape(GROUPS, 2 * TOKENS_DEV)
    onehot = (flat_ids[:, :, None] == jnp.arange(EXPERTS, dtype=jnp.int32)).astype(jnp.int32)
    position = jnp.sum((jnp.cumsum(onehot, axis=1) - 1) * onehot, axis=2)
    group_base = jnp.arange(GROUPS, dtype=jnp.int32)[:, None] * (EXPERTS * CAPACITY)
    all_slots = GROUPS * EXPERTS * CAPACITY
    slot_ids = jnp.where(position < CAPACITY, group_base + flat_ids * CAPACITY + position, all_slots).reshape(TOKENS, 2)
    token_index = jnp.broadcast_to(jnp.arange(TOKENS, dtype=jnp.int32)[:, None], (TOKENS, 2))
    source = jnp.full((all_slots,), TOKENS, dtype=jnp.int32).at[slot_ids.reshape(-1)].set(token_index.reshape(-1), mode='drop')
    buffers = jnp.take(normed, source, axis=0, mode='fill', fill_value=0)
    by_expert = buffers.reshape(GROUPS, EXPERTS, CAPACITY, D).transpose(1, 0, 2, 3).reshape(EXPERTS, GROUPS * CAPACITY, D)
    expert_out = lax.map(expert_ffn, (by_expert, w_gate, w_up, w_down))
    out_flat = expert_out.reshape(EXPERTS, GROUPS, CAPACITY, D).transpose(1, 0, 2, 3).reshape(all_slots, D)
    returned = jnp.take(out_flat, slot_ids, axis=0, mode='fill', fill_value=0)
    moe_sum = jnp.sum(gate_probs[:, :, None] * returned.astype(jnp.float32), axis=1)
    return (hidden_f32 + moe_sum).astype(jnp.bfloat16)
```

```python
import functools

import jax
import jax.numpy as jnp
from jax import lax
from jax.experimental import pallas as pl
from jax.experimental.pallas import tpu as pltpu
from jax.sharding import PartitionSpec as P

EPS = 1e-5
MESH = pl.DeviceIdType.MESH
F32 = jnp.float32
BF16 = jnp.bfloat16


def iota(shape, dim):
    return lax.broadcasted_iota(jnp.int32, shape, dim)


def moe_kernel(cfg, hid, gain, wr, wg, wu, wd, ids_row, ids_col,
               out, rhid, rg, ru, rd, stage, rows, ostage, ret,
               big, vg, vu, vd, acc, hbuf, obuf, gbuf, rbuf, ohbuf, meta, srow, rids,
               lsem, wl_sem, out_sem, ids_sem, hid_sem, w_ssem, w_rsem,
               row_ssem, row_rsem, ret_ssem, ret_rsem):
    nf, nj, per, cap, tok, dm, ff, ne = cfg
    half = dm // nf
    ndev = nf * nj
    f = lax.axis_index('fsdp')
    j = lax.axis_index('ep')
    me = f * nj + j
    of = 1 - f
    peer = {'fsdp': of, 'ep': j}

    barrier = pltpu.get_barrier_semaphore()

    @pl.loop(1, ndev)
    def _(d):
        t = lax.rem(me + d, ndev)
        pl.semaphore_signal(barrier, inc=1, device_id={'fsdp': t // nj, 'ep': lax.rem(t, nj)}, device_id_type=MESH)
    pl.semaphore_wait(barrier, ndev - 1)

    def to_peer(src, dst, s_sem, r_sem):
        return pltpu.make_async_remote_copy(src_ref=src, dst_ref=dst, send_sem=s_sem, recv_sem=r_sem,
                                            device_id=peer, device_id_type=MESH)

    ids_copy = to_peer(ids_row, rids, ids_sem.at[0], ids_sem.at[1])
    hid_copy = to_peer(hid, rhid, hid_sem.at[0], hid_sem.at[1])

    def weight_copies(i):
        return [to_peer(src.at[per * of + i], dst.at[i], w_ssem.at[3 * i + m], w_rsem.at[3 * i + m])
                for m, (src, dst) in enumerate(((wg, rg), (wu, ru), (wd, rd)))]

    ids_copy.start()
    hid_copy.start()

    @pl.loop(0, per)
    def _(i):
        for copy in weight_copies(i):
            copy.start()

    load = pltpu.make_async_copy(hid, big, lsem)
    load.start()
    load.wait()
    tt = min(256, tok)
    gain_f = gain[...].astype(F32)

    def normed_tile(rows_at):
        x = big[rows_at, :].astype(F32)
        mean_sq = jnp.mean(x * x, axis=-1, keepdims=True)
        u = (x * lax.rsqrt(mean_sq + EPS) * gain_f).astype(BF16)
        big[rows_at, :] = u
        return x, u

    lower = jnp.where(iota((tt, tt), 0) > iota((tt, tt), 1), 1.0, 0.0).astype(BF16)
    upper = jnp.where(iota((tt, tt), 0) < iota((tt, tt), 1), 1.0, 0.0).astype(BF16)

    def own_tile(t, carry):
        at = pl.ds(pl.multiple_of(t * tt, tt), tt)
        x, u = normed_tile(at)
        acc[at, :] = x
        logits = jnp.dot(u, wr[...], preferred_element_type=F32)
        lane = iota((tt, 128), 1)
        ids = ids_col[at, :]
        pick = [lane == ids[:, k:k + 1] for k in range(2)]
        count = jnp.where(pick[0] | pick[1], 1.0, 0.0)
        pos = jnp.dot(lower, count.astype(BF16), preferred_element_type=F32) + carry
        slot, score = [], []
        for k in range(2):
            place = jnp.sum(jnp.where(pick[k], pos, 0.0), axis=1, keepdims=True)
            slot.append(jnp.where(place < cap, ids[:, k:k + 1].astype(F32) * cap + place, -1.0))
            score.append(jnp.sum(jnp.where(pick[k], logits, 0.0), axis=1, keepdims=True))
        top = jnp.maximum(score[0], score[1])
        ex = [jnp.exp(s - top) for s in score]
        gate = [e / (ex[0] + ex[1]) for e in ex]
        meta[at, :] = jnp.where(lane == 0, slot[0], jnp.where(lane == 1, slot[1], jnp.where(lane == 2, gate[0], gate[1])))
        return carry + jnp.sum(count, axis=0, keepdims=True)

    lax.fori_loop(0, tok // tt, own_tile, jnp.zeros((1, 128), F32))

    def slot_rows(ids_ref):
        def tile(t, carry):
            at = pl.ds(pl.multiple_of(t * tt, tt), tt)
            sub = iota((ne, tt), 0)
            ids = [ids_ref[k:k + 1, at] for k in range(2)]
            pick = [sub == e for e in ids]
            count = jnp.where(pick[0] | pick[1], 1.0, 0.0)
            pos = jnp.dot(count.astype(BF16), upper, preferred_element_type=F32) + carry
            for k in range(2):
                place = jnp.sum(jnp.where(pick[k], pos, 0.0), axis=0, keepdims=True)
                srow[k:k + 1, at] = jnp.where(place < cap, ids[k].astype(F32) * cap + place, -1.0)
            return carry + jnp.sum(count, axis=1, keepdims=True)
        lax.fori_loop(0, tok // tt, tile, jnp.zeros((ne, 1), F32))

    tk = min(512, tok)
    tn = 256

    def pick_and_send(src, src_idx):
        @pl.loop(0, nj * per)
        def _(n):
            d, i = n // per, lax.rem(n, per)
            jo = lax.rem(j + d, nj)
            base = ((jo * nf + f) * per + i) * cap

            @pl.loop(0, tok // tk)
            def _(t):
                at = pl.ds(pl.multiple_of(t * tk, tk), tk)
                sub = iota((cap, tk), 0)
                s0 = srow[0:1, at].astype(jnp.int32) - base
                s1 = srow[1:2, at].astype(jnp.int32) - base
                ohbuf[:, at] = jnp.where((sub == s0) | (sub == s1), 1.0, 0.0).astype(BF16)

            @pl.loop(0, dm // tn)
            def _(t):
                at = pl.ds(pl.multiple_of(t * tn, tn), tn)
                gbuf[:, at] = jnp.dot(ohbuf[...], big[:, at], preferred_element_type=F32).astype(BF16)

            place = pl.ds(pl.multiple_of(src_idx * cap, cap), cap)

            @pl.when(d == 0)
            def _():
                copy = pltpu.make_async_copy(gbuf, rows.at[i, place], lsem)
                copy.start()
                copy.wait()

            @pl.when(d > 0)
            def _():
                k = src * nj * per + n
                copy = pltpu.make_async_copy(gbuf, stage.at[k], lsem)
                copy.start()
                copy.wait()
                pltpu.make_async_remote_copy(
                    src_ref=stage.at[k], dst_ref=rows.at[i, place], send_sem=row_ssem.at[k],
                    recv_sem=row_rsem.at[i * ndev + src_idx],
                    device_id={'fsdp': f, 'ep': jo}, device_id_type=MESH).start()

    slot_rows(ids_row)
    pick_and_send(0, me)

    ids_copy.wait()
    hid_copy.wait()
    load = pltpu.make_async_copy(rhid, big, lsem)
    load.start()
    load.wait()

    @pl.loop(0, tok // tt)
    def _(t):
        normed_tile(pl.ds(pl.multiple_of(t * tt, tt), tt))
    slot_rows(rids)
    pick_and_send(1, of * nj + j)

    tc = min(512, tok)

    def combine(fo, jo, i):
        e = (jo * nf + fo) * per + i

        @pl.when(fo * nj + jo != me)
        def _():
            pltpu.make_async_copy(ret.at[e], ret.at[e], ret_rsem.at[e]).wait()
        fetch = pltpu.make_async_copy(ret.at[e], rbuf, lsem)
        fetch.start()
        fetch.wait()

        @pl.loop(0, tok // tc)
        def _(t):
            at = pl.ds(pl.multiple_of(t * tc, tc), tc)
            base = (e * cap).astype(F32)
            m = meta[at, :]
            s0, s1 = m[:, 0:1] - base, m[:, 1:2] - base
            in0 = (s0 >= 0) & (s0 < cap)
            in1 = (s1 >= 0) & (s1 < cap)
            gate = jnp.where(in0, m[:, 2:3], jnp.where(in1, m[:, 3:4], 0.0))
            lane = iota((tc, cap), 1)
            hot = jnp.where((lane == s0.astype(jnp.int32)) | (lane == s1.astype(jnp.int32)), 1.0, 0.0).astype(BF16)
            acc[at, :] += gate * jnp.dot(hot, rbuf[...], preferred_element_type=F32)

    pair = 2 * cap

    @pl.loop(0, per)
    def _(i):
        mine = pl.ds(pl.multiple_of(f * half, half), half)
        theirs = pl.ds(pl.multiple_of(of * half, half), half)
        own = [pltpu.make_async_copy(wg.at[per * f + i], vg.at[mine], wl_sem.at[0]),
               pltpu.make_async_copy(wu.at[per * f + i], vu.at[mine], wl_sem.at[1]),
               pltpu.make_async_copy(wd.at[per * f + i], vd.at[:, mine], wl_sem.at[2])]
        for copy in own:
            copy.start()

        @pl.loop(0, ndev)
        def _(s):
            @pl.when(lax.rem(s, nj) != j)
            def _():
                block = rows.at[i, pl.ds(pl.multiple_of(s * cap, cap), cap)]
                pltpu.make_async_copy(block, block, row_rsem.at[i * ndev + s]).wait()
        tokens = pltpu.make_async_copy(rows.at[i], big.at[pl.ds(0, ndev * cap)], lsem)
        tokens.start()
        got = [pltpu.make_async_copy(rg.at[i], vg.at[theirs], wl_sem.at[3]),
               pltpu.make_async_copy(ru.at[i], vu.at[theirs], wl_sem.at[4]),
               pltpu.make_async_copy(rd.at[i], vd.at[:, theirs], wl_sem.at[5])]
        for remote, copy in zip(weight_copies(i), got):
            remote.wait_recv()
            copy.start()
        tokens.wait()
        for copy in own + got:
            copy.wait()

        @pl.loop(0, ndev // 2)
        def _(p):
            xs = pl.ds(pl.multiple_of(p * pair, pair), pair)

            @pl.loop(0, ff // tn)
            def _(t):
                at = pl.ds(pl.multiple_of(t * tn, tn), tn)
                a = jnp.dot(big[xs, :], vg[:, at], preferred_element_type=F32)
                b = jnp.dot(big[xs, :], vu[:, at], preferred_element_type=F32)
                hbuf[:, at] = (a * jax.nn.sigmoid(a) * b).astype(BF16)

            @pl.loop(0, dm // tn)
            def _(t):
                at = pl.ds(pl.multiple_of(t * tn, tn), tn)
                obuf[:, at] = jnp.dot(hbuf[...], vd[:, at], preferred_element_type=F32).astype(BF16)

            e = (j * nf + f) * per + i
            for q in range(2):
                s = 2 * p + q
                part = obuf.at[pl.ds(q * cap, cap)]

                @pl.when(s == me)
                def _():
                    copy = pltpu.make_async_copy(part, ret.at[e], lsem)
                    copy.start()
                    copy.wait()

                @pl.when(s != me)
                def _():
                    k = i * ndev + s
                    copy = pltpu.make_async_copy(part, ostage.at[k], lsem)
                    copy.start()
                    copy.wait()
                    pltpu.make_async_remote_copy(
                        src_ref=ostage.at[k], dst_ref=ret.at[e], send_sem=ret_ssem.at[k],
                        recv_sem=ret_rsem.at[e],
                        device_id={'fsdp': s // nj, 'ep': lax.rem(s, nj)}, device_id_type=MESH).start()

        @pl.loop(0, nj)
        def _(d):
            combine(f, lax.rem(j + d, nj), i)

    @pl.loop(0, nj * per)
    def _(n):
        combine(of, lax.rem(j + lax.rem(n, nj), nj), n // nj)

    def out_copy(t):
        at = pl.ds(pl.multiple_of(t * tc, tc), tc)
        return pltpu.make_async_copy(big.at[at], out.at[at], out_sem.at[t])

    @pl.loop(0, tok // tc)
    def _(t):
        at = pl.ds(pl.multiple_of(t * tc, tc), tc)
        big[at, :] = acc[at, :].astype(BF16)
        out_copy(t).start()

    @pl.loop(0, tok // tc)
    def _(t):
        out_copy(t).wait()

    @pl.loop(0, per)
    def _(i):
        for copy in weight_copies(i):
            copy.wait_send()

    @pl.loop(0, 2 * nj * per)
    def _(k):
        @pl.when(lax.rem(k, nj * per) >= per)
        def _():
            pltpu.make_async_copy(stage.at[k], stage.at[k], row_ssem.at[k]).wait()

    @pl.loop(0, per * ndev)
    def _(k):
        @pl.when(lax.rem(k, ndev) != me)
        def _():
            pltpu.make_async_copy(ostage.at[k], ostage.at[k], ret_ssem.at[k]).wait()


def local_block(nf, nj, hidden, norm_gain, w_router, w_gate, w_up, w_down, top2_ids):
    tok, dm = hidden.shape
    ne = w_router.shape[1]
    per = ne // (nf * nj)
    ff = w_gate.shape[2]
    cap = (5 * tok + 2 * ne - 1) // (2 * ne)
    ndev = nf * nj
    half = dm // nf
    cfg = (nf, nj, per, cap, tok, dm, ff, ne)
    ids_row = jnp.pad(top2_ids.T, ((0, 6), (0, 0)))
    router = jnp.pad(w_router, ((0, 0), (0, 128 - ne)))
    sds = jax.ShapeDtypeStruct
    anyspec = pl.BlockSpec(memory_space=pl.ANY)
    vspec = pl.BlockSpec(memory_space=pltpu.VMEM)
    outs = [
        sds((tok, dm), BF16), sds((tok, dm), BF16),
        sds((per, half, ff), BF16), sds((per, half, ff), BF16), sds((per, ff, half), BF16),
        sds((2 * nj * per, cap, dm), BF16), sds((per, ndev * cap, dm), BF16),
        sds((per * ndev, cap, dm), BF16), sds((ne, cap, dm), BF16),
    ]
    dma = pltpu.SemaphoreType.DMA
    scratch = [
        pltpu.VMEM((tok, dm), BF16),
        pltpu.VMEM((dm, ff), BF16), pltpu.VMEM((dm, ff), BF16), pltpu.VMEM((ff, dm), BF16),
        pltpu.VMEM((tok, dm), F32),
        pltpu.VMEM((2 * cap, ff), BF16), pltpu.VMEM((2 * cap, dm), BF16),
        pltpu.VMEM((cap, dm), BF16), pltpu.VMEM((cap, dm), BF16), pltpu.VMEM((cap, tok), BF16),
        pltpu.VMEM((tok, 128), F32), pltpu.VMEM((8, tok), F32), pltpu.VMEM((8, tok), jnp.int32),
        dma, dma((6,)), dma((8,)), dma((2,)), dma((2,)), dma((3 * per,)), dma((3 * per,)),
        dma((2 * nj * per,)), dma((per * ndev,)), dma((per * ndev,)), dma((ne,)),
    ]
    flops = 6 * per * ndev * cap * dm * ff + 3 * 2 * ne * cap * tok * dm
    result = pl.pallas_call(
        functools.partial(moe_kernel, cfg),
        out_shape=outs,
        in_specs=[anyspec, vspec, vspec, anyspec, anyspec, anyspec, vspec, vspec],
        out_specs=[anyspec] * len(outs),
        scratch_shapes=scratch,
        compiler_params=pltpu.CompilerParams(collective_id=0, has_side_effects=True, vmem_limit_bytes=67043328),
        cost_estimate=pl.CostEstimate(flops=flops, bytes_accessed=400 * 1024 * 1024, transcendentals=0),
        name='moe_block',
    )(hidden, norm_gain.reshape(1, dm), router, w_gate, w_up, w_down, ids_row, top2_ids)
    return result[0]


def solution(mesh):
    tok_spec = P(('dp', 'fsdp', 'ep'), None)
    in_specs = (tok_spec, P(None), P(None, None), P('ep', 'fsdp', None), P('ep', 'fsdp', None), P('ep', None, 'fsdp'), tok_spec)
    body = functools.partial(local_block, mesh.shape['fsdp'], mesh.shape['ep'])
    return jax.shard_map(body, mesh=mesh, in_specs=in_specs, out_specs=tok_spec, check_vma=False)
```

```python
import functools

import jax
import jax.numpy as jnp
from jax import lax
from jax.experimental import pallas as pl
from jax.experimental.pallas import tpu as pltpu
from jax.sharding import PartitionSpec as P

EPS = 1e-5
MESH = pl.DeviceIdType.MESH
F32 = jnp.float32
BF16 = jnp.bfloat16


def iota(shape, dim):
    return lax.broadcasted_iota(jnp.int32, shape, dim)


def moe_kernel(cfg, hid, gain, wr, wg, wu, wd, ids_row,
               out, rhid, rg, ru, rd, stage, rows, ostage, ret,
               big, vg, vu, vd, acc, hbuf, obuf, gbuf, rbuf, ohbuf, meta, srow, rids,
               lsem, wl_sem, tok_sem, out_sem, ids_sem, hid_sem, w_ssem, w_rsem,
               row_ssem, row_rsem, ret_ssem, ret_rsem):
    nf, nj, per, cap, tok, dm, ff, ne = cfg
    half = dm // nf
    ndev = nf * nj
    f = lax.axis_index('fsdp')
    j = lax.axis_index('ep')
    me = f * nj + j
    of = 1 - f
    peer = {'fsdp': of, 'ep': j}

    barrier = pltpu.get_barrier_semaphore()

    @pl.loop(1, ndev)
    def _(d):
        t = lax.rem(me + d, ndev)
        pl.semaphore_signal(barrier, inc=1, device_id={'fsdp': t // nj, 'ep': lax.rem(t, nj)}, device_id_type=MESH)
    pl.semaphore_wait(barrier, ndev - 1)

    def to_peer(src, dst, s_sem, r_sem):
        return pltpu.make_async_remote_copy(src_ref=src, dst_ref=dst, send_sem=s_sem, recv_sem=r_sem,
                                            device_id=peer, device_id_type=MESH)

    ids_copy = to_peer(ids_row, rids, ids_sem.at[0], ids_sem.at[1])
    hid_copy = to_peer(hid, rhid, hid_sem.at[0], hid_sem.at[1])

    def weight_copies(i):
        return [to_peer(src.at[per * of + i], dst.at[i], w_ssem.at[3 * i + m], w_rsem.at[3 * i + m])
                for m, (src, dst) in enumerate(((wg, rg), (wu, ru), (wd, rd)))]

    ids_copy.start()
    hid_copy.start()

    @pl.loop(0, per)
    def _(i):
        for copy in weight_copies(i):
            copy.start()

    load = pltpu.make_async_copy(hid, big, lsem)
    load.start()
    load.wait()
    tt = min(256, tok)
    router = jnp.concatenate([wr[...], jnp.zeros((128 - ne, dm), BF16)], axis=0)
    gain_f = gain[...].astype(F32)

    def normed_tile(rows_at):
        x = big[rows_at, :].astype(F32)
        mean_sq = jnp.mean(x * x, axis=-1, keepdims=True)
        u = (x * lax.rsqrt(mean_sq + EPS) * gain_f).astype(BF16)
        big[rows_at, :] = u
        return x, u

    upper = jnp.where(iota((tt, tt), 0) < iota((tt, tt), 1), 1.0, 0.0).astype(BF16)

    def slot_rows(ids_ref):
        def tile(t, carry):
            at = pl.ds(pl.multiple_of(t * tt, tt), tt)
            sub = iota((ne, tt), 0)
            ids = [ids_ref[k:k + 1, at] for k in range(2)]
            pick = [sub == e for e in ids]
            count = jnp.where(pick[0] | pick[1], 1.0, 0.0)
            pos = jnp.dot(count.astype(BF16), upper, preferred_element_type=F32) + carry
            for k in range(2):
                place = jnp.sum(jnp.where(pick[k], pos, 0.0), axis=0, keepdims=True)
                srow[k:k + 1, at] = jnp.where(place < cap, ids[k].astype(F32) * cap + place, -1.0)
            return carry + jnp.sum(count, axis=1, keepdims=True)
        lax.fori_loop(0, tok // tt, tile, jnp.zeros((ne, 1), F32))

    def own_tile(t):
        at = pl.ds(pl.multiple_of(t * tt, tt), tt)
        x, u = normed_tile(at)
        acc[at, :] = x
        logits = lax.dot_general(u, router, (((1,), (1,)), ((), ())), preferred_element_type=F32)
        lane = iota((tt, 128), 1)
        eye = iota((tt, tt), 0) == iota((tt, tt), 1)

        def column(row):
            return jnp.sum(jnp.where(eye, row, 0.0), axis=1, keepdims=True)
        slot = [column(srow[k:k + 1, at]) for k in range(2)]
        ids = [column(ids_row[k:k + 1, at].astype(F32)).astype(jnp.int32) for k in range(2)]
        score = [jnp.sum(jnp.where(lane == e, logits, 0.0), axis=1, keepdims=True) for e in ids]
        top = jnp.maximum(score[0], score[1])
        ex = [jnp.exp(v - top) for v in score]
        gate = [v / (ex[0] + ex[1]) for v in ex]
        meta[at, :] = jnp.where(lane == 0, slot[0], jnp.where(lane == 1, slot[1], jnp.where(lane == 2, gate[0], gate[1])))

    tk = min(512, tok)
    tn = 256

    def pick_and_send(src, src_idx):
        @pl.loop(0, nj * per)
        def _(n):
            d, i = n // per, lax.rem(n, per)
            jo = lax.rem(j + d, nj)
            base = ((jo * nf + f) * per + i) * cap

            @pl.loop(0, tok // tk)
            def _(t):
                at = pl.ds(pl.multiple_of(t * tk, tk), tk)
                sub = iota((cap, tk), 0)
                s0 = srow[0:1, at].astype(jnp.int32) - base
                s1 = srow[1:2, at].astype(jnp.int32) - base
                ohbuf[:, at] = jnp.where((sub == s0) | (sub == s1), 1.0, 0.0).astype(BF16)

            @pl.loop(0, dm // tn)
            def _(t):
                at = pl.ds(pl.multiple_of(t * tn, tn), tn)
                gbuf[:, at] = jnp.dot(ohbuf[...], big[:, at], preferred_element_type=F32).astype(BF16)

            place = pl.ds(pl.multiple_of(src_idx * cap, cap), cap)

            @pl.when(d == 0)
            def _():
                copy = pltpu.make_async_copy(gbuf, rows.at[i, place], lsem)
                copy.start()
                copy.wait()

            @pl.when(d > 0)
            def _():
                k = src * nj * per + n
                copy = pltpu.make_async_copy(gbuf, stage.at[k], lsem)
                copy.start()
                copy.wait()
                pltpu.make_async_remote_copy(
                    src_ref=stage.at[k], dst_ref=rows.at[i, place], send_sem=row_ssem.at[k],
                    recv_sem=row_rsem.at[i * ndev + src_idx],
                    device_id={'fsdp': f, 'ep': jo}, device_id_type=MESH).start()

    slot_rows(ids_row)
    pl.loop(0, tok // tt)(own_tile)
    pick_and_send(0, me)

    ids_copy.wait()
    hid_copy.wait()
    load = pltpu.make_async_copy(rhid, big, lsem)
    load.start()
    load.wait()

    @pl.loop(0, tok // tt)
    def _(t):
        normed_tile(pl.ds(pl.multiple_of(t * tt, tt), tt))
    slot_rows(rids)
    pick_and_send(1, of * nj + j)

    tc = min(512, tok)

    def out_copy(t):
        at = pl.ds(pl.multiple_of(t * tc, tc), tc)
        return pltpu.make_async_copy(big.at[at], out.at[at], out_sem.at[t])

    def combine(fo, jo, i, last=False):
        e = (jo * nf + fo) * per + i

        @pl.when(fo * nj + jo != me)
        def _():
            pltpu.make_async_copy(ret.at[e], ret.at[e], ret_rsem.at[e]).wait()
        fetch = pltpu.make_async_copy(ret.at[e], rbuf, lsem)
        fetch.start()
        fetch.wait()

        @pl.loop(0, tok // tc)
        def _(t):
            at = pl.ds(pl.multiple_of(t * tc, tc), tc)
            base = (e * cap).astype(F32)
            m = meta[at, :]
            s0, s1 = m[:, 0:1] - base, m[:, 1:2] - base
            in0 = (s0 >= 0) & (s0 < cap)
            in1 = (s1 >= 0) & (s1 < cap)
            gate = jnp.where(in0, m[:, 2:3], jnp.where(in1, m[:, 3:4], 0.0))
            lane = iota((tc, cap), 1)
            hot = jnp.where((lane == s0.astype(jnp.int32)) | (lane == s1.astype(jnp.int32)), 1.0, 0.0).astype(BF16)
            total = acc[at, :] + gate * jnp.dot(hot, rbuf[...], preferred_element_type=F32)
            if last:
                big[at, :] = total.astype(BF16)
                out_copy(t).start()
            else:
                acc[at, :] = total

    pair = 2 * cap

    def source(n):
        return jnp.where(n < nj, of, f) * nj + lax.rem(j + n, nj)

    @pl.loop(0, per)
    def _(i):
        mine = pl.ds(pl.multiple_of(f * half, half), half)
        theirs = pl.ds(pl.multiple_of(of * half, half), half)
        own = [pltpu.make_async_copy(wg.at[per * f + i], vg.at[mine], wl_sem.at[0]),
               pltpu.make_async_copy(wu.at[per * f + i], vu.at[mine], wl_sem.at[1]),
               pltpu.make_async_copy(wd.at[per * f + i], vd.at[:, mine], wl_sem.at[2])]
        for copy in own:
            copy.start()

        def tokens(n):
            return pltpu.make_async_copy(rows.at[i, pl.ds(pl.multiple_of(source(n) * cap, cap), cap)],
                                         big.at[pl.ds(pl.multiple_of(n * cap, cap), cap)], tok_sem.at[n])

        @pl.loop(0, ndev)
        def _(n):
            s = source(n)

            @pl.when(lax.rem(s, nj) != j)
            def _():
                block = rows.at[i, pl.ds(pl.multiple_of(s * cap, cap), cap)]
                pltpu.make_async_copy(block, block, row_rsem.at[i * ndev + s]).wait()
            tokens(n).start()
        got = [pltpu.make_async_copy(rg.at[i], vg.at[theirs], wl_sem.at[3]),
               pltpu.make_async_copy(ru.at[i], vu.at[theirs], wl_sem.at[4]),
               pltpu.make_async_copy(rd.at[i], vd.at[:, theirs], wl_sem.at[5])]
        for remote, copy in zip(weight_copies(i), got):
            remote.wait_recv()
            copy.start()

        @pl.loop(0, ndev)
        def _(n):
            tokens(n).wait()
        for copy in own + got:
            copy.wait()

        @pl.loop(0, ndev // 2)
        def _(p):
            xs = pl.ds(pl.multiple_of(p * pair, pair), pair)

            @pl.loop(0, ff // tn)
            def _(t):
                at = pl.ds(pl.multiple_of(t * tn, tn), tn)
                a = jnp.dot(big[xs, :], vg[:, at], preferred_element_type=F32)
                b = jnp.dot(big[xs, :], vu[:, at], preferred_element_type=F32)
                hbuf[:, at] = (a * jax.nn.sigmoid(a) * b).astype(BF16)

            @pl.loop(0, dm // tn)
            def _(t):
                at = pl.ds(pl.multiple_of(t * tn, tn), tn)
                obuf[:, at] = jnp.dot(hbuf[...], vd[:, at], preferred_element_type=F32).astype(BF16)

            e = (j * nf + f) * per + i
            for q in range(2):
                s = source(2 * p + q)
                part = obuf.at[pl.ds(q * cap, cap)]

                @pl.when(s == me)
                def _():
                    copy = pltpu.make_async_copy(part, ret.at[e], lsem)
                    copy.start()
                    copy.wait()

                @pl.when(s != me)
                def _():
                    k = i * ndev + s
                    copy = pltpu.make_async_copy(part, ostage.at[k], lsem)
                    copy.start()
                    copy.wait()
                    pltpu.make_async_remote_copy(
                        src_ref=ostage.at[k], dst_ref=ret.at[e], send_sem=ret_ssem.at[k],
                        recv_sem=ret_rsem.at[e],
                        device_id={'fsdp': s // nj, 'ep': lax.rem(s, nj)}, device_id_type=MESH).start()

        @pl.loop(0, nj)
        def _(d):
            combine(f, lax.rem(j + nj - d, nj), i)

    @pl.loop(0, nj * per - 1)
    def _(n):
        combine(of, lax.rem(j + nj - lax.rem(n, nj), nj), n // nj)
    combine(of, lax.rem(j + 1, nj), per - 1, last=True)

    @pl.loop(0, tok // tc)
    def _(t):
        out_copy(t).wait()

    @pl.loop(0, per)
    def _(i):
        for copy in weight_copies(i):
            copy.wait_send()

    @pl.loop(0, 2 * nj * per)
    def _(k):
        @pl.when(lax.rem(k, nj * per) >= per)
        def _():
            pltpu.make_async_copy(stage.at[k], stage.at[k], row_ssem.at[k]).wait()

    @pl.loop(0, per * ndev)
    def _(k):
        @pl.when(lax.rem(k, ndev) != me)
        def _():
            pltpu.make_async_copy(ostage.at[k], ostage.at[k], ret_ssem.at[k]).wait()


def local_block(nf, nj, hidden, norm_gain, w_router, w_gate, w_up, w_down, top2_ids):
    tok, dm = hidden.shape
    ne = w_router.shape[1]
    per = ne // (nf * nj)
    ff = w_gate.shape[2]
    cap = (5 * tok + 2 * ne - 1) // (2 * ne)
    ndev = nf * nj
    half = dm // nf
    cfg = (nf, nj, per, cap, tok, dm, ff, ne)
    sds = jax.ShapeDtypeStruct
    anyspec = pl.BlockSpec(memory_space=pl.ANY)
    vspec = pl.BlockSpec(memory_space=pltpu.VMEM)
    outs = [
        sds((tok, dm), BF16), sds((tok, dm), BF16),
        sds((per, half, ff), BF16), sds((per, half, ff), BF16), sds((per, ff, half), BF16),
        sds((2 * nj * per, cap, dm), BF16), sds((per, ndev * cap, dm), BF16),
        sds((per * ndev, cap, dm), BF16), sds((ne, cap, dm), BF16),
    ]
    dma = pltpu.SemaphoreType.DMA
    scratch = [
        pltpu.VMEM((tok, dm), BF16),
        pltpu.VMEM((dm, ff), BF16), pltpu.VMEM((dm, ff), BF16), pltpu.VMEM((ff, dm), BF16),
        pltpu.VMEM((tok, dm), F32),
        pltpu.VMEM((2 * cap, ff), BF16), pltpu.VMEM((2 * cap, dm), BF16),
        pltpu.VMEM((cap, dm), BF16), pltpu.VMEM((cap, dm), BF16), pltpu.VMEM((cap, tok), BF16),
        pltpu.VMEM((tok, 128), F32), pltpu.VMEM((8, tok), F32), pltpu.VMEM((2, tok), jnp.int32),
        dma, dma((6,)), dma((ndev,)), dma((8,)), dma((2,)), dma((2,)), dma((3 * per,)), dma((3 * per,)),
        dma((2 * nj * per,)), dma((per * ndev,)), dma((per * ndev,)), dma((ne,)),
    ]
    flops = 6 * per * ndev * cap * dm * ff + 3 * 2 * ne * cap * tok * dm
    result = pl.pallas_call(
        functools.partial(moe_kernel, cfg),
        out_shape=outs,
        in_specs=[anyspec, vspec, vspec, anyspec, anyspec, anyspec, vspec],
        out_specs=[anyspec] * len(outs),
        scratch_shapes=scratch,
        compiler_params=pltpu.CompilerParams(collective_id=0, has_side_effects=True, vmem_limit_bytes=67043328),
        cost_estimate=pl.CostEstimate(flops=flops, bytes_accessed=400 * 1024 * 1024, transcendentals=0),
        name='moe_block',
    )(hidden, norm_gain.reshape(1, dm), w_router.T, w_gate, w_up, w_down, top2_ids.T)
    return result[0]


def solution(mesh):
    tok_spec = P(('dp', 'fsdp', 'ep'), None)
    in_specs = (tok_spec, P(None), P(None, None), P('ep', 'fsdp', None), P('ep', 'fsdp', None), P('ep', None, 'fsdp'), tok_spec)
    body = functools.partial(local_block, mesh.shape['fsdp'], mesh.shape['ep'])
    return jax.shard_map(body, mesh=mesh, in_specs=in_specs, out_specs=tok_spec, check_vma=False)
```

```python
import functools

import jax
import jax.numpy as jnp
from jax import lax
from jax.experimental import pallas as pl
from jax.experimental.pallas import tpu as pltpu
from jax.sharding import PartitionSpec as P

EPS = 1e-5
MESH = pl.DeviceIdType.MESH
F32 = jnp.float32
BF16 = jnp.bfloat16


def iota(shape, dim):
    return lax.broadcasted_iota(jnp.int32, shape, dim)


def add_expert(total, m, block, e, cap):
    base = (e * cap).astype(F32)
    s0, s1 = m[:, 0:1] - base, m[:, 1:2] - base
    in0 = (s0 >= 0) & (s0 < cap)
    in1 = (s1 >= 0) & (s1 < cap)
    gate = jnp.where(in0, m[:, 2:3], jnp.where(in1, m[:, 3:4], 0.0))
    lane = iota((m.shape[0], cap), 1)
    hot = jnp.where((lane == s0.astype(jnp.int32)) | (lane == s1.astype(jnp.int32)), 1.0, 0.0).astype(BF16)
    return total + gate * jnp.dot(hot, block, preferred_element_type=F32)


def last_kernel(nf, nj, per, cap, acc, meta, ret, out):
    f, j = lax.axis_index('fsdp'), lax.axis_index('ep')
    e = (lax.rem(j + 1, nj) * nf + 1 - f) * per + per - 1
    out[...] = add_expert(acc[...], meta[...], ret[0], e, cap).astype(BF16)


def moe_kernel(cfg, hid, gain, wr, wg, wu, wd, ids_row,
               acc_out, meta_out, rhid, rg, ru, rd, stage, rows, ostage, ret,
               big, vg, vu, vd, acc, hbuf, obuf, gbuf, rbuf, ohbuf, meta, srow, rids,
               lsem, wl_sem, tok_sem, out_sem, ids_sem, hid_sem, w_ssem, w_rsem,
               row_ssem, row_rsem, ret_ssem, ret_rsem):
    nf, nj, per, cap, tok, dm, ff, ne = cfg
    half = dm // nf
    ndev = nf * nj
    f = lax.axis_index('fsdp')
    j = lax.axis_index('ep')
    me = f * nj + j
    of = 1 - f
    peer = {'fsdp': of, 'ep': j}

    barrier = pltpu.get_barrier_semaphore()

    @pl.loop(1, ndev)
    def _(d):
        t = lax.rem(me + d, ndev)
        pl.semaphore_signal(barrier, inc=1, device_id={'fsdp': t // nj, 'ep': lax.rem(t, nj)}, device_id_type=MESH)
    pl.semaphore_wait(barrier, ndev - 1)

    def to_peer(src, dst, s_sem, r_sem):
        return pltpu.make_async_remote_copy(src_ref=src, dst_ref=dst, send_sem=s_sem, recv_sem=r_sem,
                                            device_id=peer, device_id_type=MESH)

    ids_copy = to_peer(ids_row, rids, ids_sem.at[0], ids_sem.at[1])
    hid_copy = to_peer(hid, rhid, hid_sem.at[0], hid_sem.at[1])

    def weight_copies(i):
        return [to_peer(src.at[per * of + i], dst.at[i], w_ssem.at[3 * i + m], w_rsem.at[3 * i + m])
                for m, (src, dst) in enumerate(((wg, rg), (wu, ru), (wd, rd)))]

    ids_copy.start()
    hid_copy.start()

    @pl.loop(0, per)
    def _(i):
        for copy in weight_copies(i):
            copy.start()

    load = pltpu.make_async_copy(hid, big, lsem)
    load.start()
    load.wait()
    tt = min(256, tok)
    router = jnp.concatenate([wr[...], jnp.zeros((128 - ne, dm), BF16)], axis=0)
    gain_8 = gain[...].astype(F32)
    gain_f = jnp.concatenate([gain_8[k:k + 1, :] for k in range(gain_8.shape[0])], axis=1)

    def normed_tile(rows_at):
        x = big[rows_at, :].astype(F32)
        mean_sq = jnp.mean(x * x, axis=-1, keepdims=True)
        u = (x * lax.rsqrt(mean_sq + EPS) * gain_f).astype(BF16)
        big[rows_at, :] = u
        return x, u

    upper = jnp.where(iota((tt, tt), 0) < iota((tt, tt), 1), 1.0, 0.0).astype(BF16)

    def slot_rows(ids_ref):
        def tile(t, carry):
            at = pl.ds(pl.multiple_of(t * tt, tt), tt)
            sub = iota((ne, tt), 0)
            ids = [ids_ref[k:k + 1, at] for k in range(2)]
            pick = [sub == e for e in ids]
            count = jnp.where(pick[0] | pick[1], 1.0, 0.0)
            pos = jnp.dot(count.astype(BF16), upper, preferred_element_type=F32) + carry
            for k in range(2):
                place = jnp.sum(jnp.where(pick[k], pos, 0.0), axis=0, keepdims=True)
                srow[k:k + 1, at] = jnp.where(place < cap, ids[k].astype(F32) * cap + place, -1.0)
            return carry + jnp.sum(count, axis=1, keepdims=True)
        lax.fori_loop(0, tok // tt, tile, jnp.zeros((ne, 1), F32))

    def own_tile(t):
        at = pl.ds(pl.multiple_of(t * tt, tt), tt)
        x, u = normed_tile(at)
        acc[at, :] = x
        logits = lax.dot_general(u, router, (((1,), (1,)), ((), ())), preferred_element_type=F32)
        lane = iota((tt, 128), 1)
        eye = iota((tt, tt), 0) == iota((tt, tt), 1)

        def column(row):
            return jnp.sum(jnp.where(eye, row, 0.0), axis=1, keepdims=True)
        slot = [column(srow[k:k + 1, at]) for k in range(2)]
        ids = [column(ids_row[k:k + 1, at].astype(F32)).astype(jnp.int32) for k in range(2)]
        score = [jnp.sum(jnp.where(lane == e, logits, 0.0), axis=1, keepdims=True) for e in ids]
        top = jnp.maximum(score[0], score[1])
        ex = [jnp.exp(v - top) for v in score]
        gate = [v / (ex[0] + ex[1]) for v in ex]
        meta[at, :] = jnp.where(lane == 0, slot[0], jnp.where(lane == 1, slot[1], jnp.where(lane == 2, gate[0], gate[1])))

    tk = min(512, tok)
    tn = 256

    def pick_and_send(src, src_idx):
        @pl.loop(0, nj * per)
        def _(n):
            d, i = n // per, lax.rem(n, per)
            jo = lax.rem(j + d, nj)
            base = ((jo * nf + f) * per + i) * cap

            @pl.loop(0, tok // tk)
            def _(t):
                at = pl.ds(pl.multiple_of(t * tk, tk), tk)
                sub = iota((cap, tk), 0)
                s0 = srow[0:1, at].astype(jnp.int32) - base
                s1 = srow[1:2, at].astype(jnp.int32) - base
                ohbuf[:, at] = jnp.where((sub == s0) | (sub == s1), 1.0, 0.0).astype(BF16)

            @pl.loop(0, dm // tn)
            def _(t):
                at = pl.ds(pl.multiple_of(t * tn, tn), tn)
                gbuf[:, at] = jnp.dot(ohbuf[...], big[:, at], preferred_element_type=F32).astype(BF16)

            place = pl.ds(pl.multiple_of(src_idx * cap, cap), cap)

            @pl.when(d == 0)
            def _():
                copy = pltpu.make_async_copy(gbuf, rows.at[i, place], lsem)
                copy.start()
                copy.wait()

            @pl.when(d > 0)
            def _():
                k = src * nj * per + n
                copy = pltpu.make_async_copy(gbuf, stage.at[k], lsem)
                copy.start()
                copy.wait()
                pltpu.make_async_remote_copy(
                    src_ref=stage.at[k], dst_ref=rows.at[i, place], send_sem=row_ssem.at[k],
                    recv_sem=row_rsem.at[i * ndev + src_idx],
                    device_id={'fsdp': f, 'ep': jo}, device_id_type=MESH).start()

    slot_rows(ids_row)
    pl.loop(0, tok // tt)(own_tile)
    pick_and_send(0, me)

    ids_copy.wait()
    hid_copy.wait()
    load = pltpu.make_async_copy(rhid, big, lsem)
    load.start()
    load.wait()

    @pl.loop(0, tok // tt)
    def _(t):
        normed_tile(pl.ds(pl.multiple_of(t * tt, tt), tt))
    slot_rows(rids)
    pick_and_send(1, of * nj + j)

    tc = min(512, tok)

    def arrival(side, d, i):
        return (side * nj + d) * per + i

    def combine(side, d, i):
        fo, jo = jnp.where(side == 1, of, f), lax.rem(j + nj - d, nj)
        r = arrival(side, d, i)

        @pl.when(fo * nj + jo != me)
        def _():
            pltpu.make_async_copy(ret.at[r], ret.at[r], ret_rsem.at[r]).wait()
        fetch = pltpu.make_async_copy(ret.at[r], rbuf, lsem)
        fetch.start()
        fetch.wait()

        @pl.loop(0, tok // tc)
        def _(t):
            at = pl.ds(pl.multiple_of(t * tc, tc), tc)
            acc[at, :] = add_expert(acc[at, :], meta[at, :], rbuf[...], (jo * nf + fo) * per + i, cap)

    pair = 2 * cap

    def source(n):
        return jnp.where(n < nj, of, f) * nj + lax.rem(j + n, nj)

    @pl.loop(0, per)
    def _(i):
        mine = pl.ds(pl.multiple_of(f * half, half), half)
        theirs = pl.ds(pl.multiple_of(of * half, half), half)
        own = [pltpu.make_async_copy(wg.at[per * f + i], vg.at[mine], wl_sem.at[0]),
               pltpu.make_async_copy(wu.at[per * f + i], vu.at[mine], wl_sem.at[1]),
               pltpu.make_async_copy(wd.at[per * f + i], vd.at[:, mine], wl_sem.at[2])]
        for copy in own:
            copy.start()

        def tokens(n):
            return pltpu.make_async_copy(rows.at[i, pl.ds(pl.multiple_of(source(n) * cap, cap), cap)],
                                         big.at[pl.ds(pl.multiple_of(n * cap, cap), cap)], tok_sem.at[n])

        @pl.loop(0, ndev)
        def _(n):
            s = source(n)

            @pl.when(lax.rem(s, nj) != j)
            def _():
                block = rows.at[i, pl.ds(pl.multiple_of(s * cap, cap), cap)]
                pltpu.make_async_copy(block, block, row_rsem.at[i * ndev + s]).wait()
            tokens(n).start()
        got = [pltpu.make_async_copy(rg.at[i], vg.at[theirs], wl_sem.at[3]),
               pltpu.make_async_copy(ru.at[i], vu.at[theirs], wl_sem.at[4]),
               pltpu.make_async_copy(rd.at[i], vd.at[:, theirs], wl_sem.at[5])]
        for remote, copy in zip(weight_copies(i), got):
            remote.wait_recv()
            copy.start()

        @pl.loop(0, ndev)
        def _(n):
            tokens(n).wait()
        for copy in own + got:
            copy.wait()

        @pl.loop(0, ndev // 2)
        def _(p):
            xs = pl.ds(pl.multiple_of(p * pair, pair), pair)

            @pl.loop(0, ff // tn)
            def _(t):
                at = pl.ds(pl.multiple_of(t * tn, tn), tn)
                a = jnp.dot(big[xs, :], vg[:, at], preferred_element_type=F32)
                b = jnp.dot(big[xs, :], vu[:, at], preferred_element_type=F32)
                hbuf[:, at] = (a * jax.nn.sigmoid(a) * b).astype(BF16)

            @pl.loop(0, dm // tn)
            def _(t):
                at = pl.ds(pl.multiple_of(t * tn, tn), tn)
                obuf[:, at] = jnp.dot(hbuf[...], vd[:, at], preferred_element_type=F32).astype(BF16)

            for q in range(2):
                n = 2 * p + q
                s = source(n)
                r = arrival(jnp.where(n < nj, 1, 0), lax.rem(n, nj), i)
                part = obuf.at[pl.ds(q * cap, cap)]

                @pl.when(s == me)
                def _():
                    copy = pltpu.make_async_copy(part, ret.at[r], lsem)
                    copy.start()
                    copy.wait()

                @pl.when(s != me)
                def _():
                    k = i * ndev + s
                    copy = pltpu.make_async_copy(part, ostage.at[k], lsem)
                    copy.start()
                    copy.wait()
                    pltpu.make_async_remote_copy(
                        src_ref=ostage.at[k], dst_ref=ret.at[r], send_sem=ret_ssem.at[k],
                        recv_sem=ret_rsem.at[r],
                        device_id={'fsdp': s // nj, 'ep': lax.rem(s, nj)}, device_id_type=MESH).start()

        @pl.loop(0, nj)
        def _(d):
            combine(0, d, i)

    meta_copy = pltpu.make_async_copy(meta, meta_out, out_sem.at[1])
    meta_copy.start()

    @pl.loop(0, nj * per - 1)
    def _(n):
        combine(1, lax.rem(n, nj), n // nj)
    acc_copy = pltpu.make_async_copy(acc, acc_out, out_sem.at[0])
    acc_copy.start()
    meta_copy.wait()
    acc_copy.wait()

    @pl.loop(0, per)
    def _(i):
        for copy in weight_copies(i):
            copy.wait_send()

    @pl.loop(0, 2 * nj * per)
    def _(k):
        @pl.when(lax.rem(k, nj * per) >= per)
        def _():
            pltpu.make_async_copy(stage.at[k], stage.at[k], row_ssem.at[k]).wait()

    @pl.loop(0, per * ndev)
    def _(k):
        @pl.when(lax.rem(k, ndev) != me)
        def _():
            pltpu.make_async_copy(ostage.at[k], ostage.at[k], ret_ssem.at[k]).wait()


    pltpu.make_async_copy(ret.at[ne - 1], ret.at[ne - 1], ret_rsem.at[ne - 1]).wait()


def local_block(nf, nj, hidden, norm_gain, w_router, w_gate, w_up, w_down, top2_ids):
    tok, dm = hidden.shape
    ne = w_router.shape[1]
    per = ne // (nf * nj)
    ff = w_gate.shape[2]
    cap = (5 * tok + 2 * ne - 1) // (2 * ne)
    ndev = nf * nj
    half = dm // nf
    cfg = (nf, nj, per, cap, tok, dm, ff, ne)
    sds = jax.ShapeDtypeStruct
    anyspec = pl.BlockSpec(memory_space=pl.ANY)
    vspec = pl.BlockSpec(memory_space=pltpu.VMEM)
    outs = [
        sds((tok, dm), F32), sds((tok, 128), F32), sds((tok, dm), BF16),
        sds((per, half, ff), BF16), sds((per, half, ff), BF16), sds((per, ff, half), BF16),
        sds((2 * nj * per, cap, dm), BF16), sds((per, ndev * cap, dm), BF16),
        sds((per * ndev, cap, dm), BF16), sds((ne, cap, dm), BF16),
    ]
    dma = pltpu.SemaphoreType.DMA
    scratch = [
        pltpu.VMEM((tok, dm), BF16),
        pltpu.VMEM((dm, ff), BF16), pltpu.VMEM((dm, ff), BF16), pltpu.VMEM((ff, dm), BF16),
        pltpu.VMEM((tok, dm), F32),
        pltpu.VMEM((2 * cap, ff), BF16), pltpu.VMEM((2 * cap, dm), BF16),
        pltpu.VMEM((cap, dm), BF16), pltpu.VMEM((cap, dm), BF16), pltpu.VMEM((cap, tok), BF16),
        pltpu.VMEM((tok, 128), F32), pltpu.VMEM((8, tok), F32), pltpu.VMEM((2, tok), jnp.int32),
        dma, dma((6,)), dma((ndev,)), dma((2,)), dma((2,)), dma((2,)), dma((3 * per,)), dma((3 * per,)),
        dma((2 * nj * per,)), dma((per * ndev,)), dma((per * ndev,)), dma((ne,)),
    ]
    flops = 6 * per * ndev * cap * dm * ff + 3 * 2 * ne * cap * tok * dm
    acc, meta, *_, ret = pl.pallas_call(
        functools.partial(moe_kernel, cfg),
        out_shape=outs,
        in_specs=[anyspec, vspec, vspec, anyspec, anyspec, anyspec, vspec],
        out_specs=[anyspec] * len(outs),
        scratch_shapes=scratch,
        compiler_params=pltpu.CompilerParams(collective_id=0, has_side_effects=True, vmem_limit_bytes=67043328),
        cost_estimate=pl.CostEstimate(flops=flops, bytes_accessed=400 * 1024 * 1024, transcendentals=0),
        name='moe_block',
    )(hidden, norm_gain.reshape(dm // 128, 128), w_router.T, w_gate, w_up, w_down, top2_ids.T)
    tc = min(512, tok)
    return pl.pallas_call(
        functools.partial(last_kernel, nf, nj, per, cap),
        out_shape=sds((tok, dm), BF16),
        grid=(tok // tc,),
        in_specs=[pl.BlockSpec((tc, dm), lambda t: (t, 0)), pl.BlockSpec((tc, 128), lambda t: (t, 0)),
                  pl.BlockSpec((1, cap, dm), lambda t: (ne - 1, 0, 0))],
        out_specs=pl.BlockSpec((tc, dm), lambda t: (t, 0)),
        cost_estimate=pl.CostEstimate(flops=2 * tok * cap * dm, bytes_accessed=26 * 1024 * 1024, transcendentals=0),
        name='moe_last',
    )(acc, meta, ret)


def solution(mesh):
    tok_spec = P(('dp', 'fsdp', 'ep'), None)
    in_specs = (tok_spec, P(None), P(None, None), P('ep', 'fsdp', None), P('ep', 'fsdp', None), P('ep', None, 'fsdp'), tok_spec)
    body = functools.partial(local_block, mesh.shape['fsdp'], mesh.shape['ep'])
    return jax.shard_map(body, mesh=mesh, in_specs=in_specs, out_specs=tok_spec, check_vma=False)
```
